8 devices in a mesh: rep: 1 (over z), dp: 8 (over x, y, core).
Axes of the slice: x: 2, y: 2, z: 1, core: 2. Of those that a mesh axis runs over, the one named last changes fastest.
Arguments:
- x: bfloat16 [8, 2048, 1280], P(('rep', 'dp'))
- dy: bfloat16 [8, 2048, 1280], P(('rep', 'dp'))
- w_gate: bfloat16 [2, 1280, 4480], P(None, 'dp')
- w_up: bfloat16 [2, 1280, 4480], P(None, 'dp')
- w_down: bfloat16 [2, 4480, 1280], P(None, 'dp')
- m_w_gate: float32 [2, 1280, 4480], P(None, 'dp')
- m_w_up: float32 [2, 1280, 4480], P(None, 'dp')
- m_w_down: float32 [2, 4480, 1280], P(None, 'dp')
- v_w_gate: float32 [2, 1280, 4480], P(None, 'dp')
- v_w_up: float32 [2, 1280, 4480], P(None, 'dp')
- v_w_down: float32 [2, 4480, 1280], P(None, 'dp')
Outputs:
- output 1: bfloat16 [2, 1280, 4480], P('rep', 'dp')
- output 2: bfloat16 [2, 1280, 4480], P('rep', 'dp')
- output 3: bfloat16 [2, 4480, 1280], P('rep', 'dp')
- output 4: float32 [2, 1280, 4480], P('rep', 'dp')
- output 5: float32 [2, 1280, 4480], P('rep', 'dp')
- output 6: float32 [2, 4480, 1280], P('rep', 'dp')
- output 7: float32 [2, 1280, 4480], P('rep', 'dp')
- output 8: float32 [2, 1280, 4480], P('rep', 'dp')
- output 9: float32 [2, 4480, 1280], P('rep', 'dp')
All inputs are finite; a program needn't handle non-finite values.
Results may differ from the reference program's by a relative error of at most 0.022.
Values are sent between devices in bfloat16 or wider.
A program may use at most 2 GiB of HBM per device.

```python
import jax
import jax.numpy as jnp
from jax import lax

SEQUENCES = 8
TOKENS = 2048
D = 1280
FF = 4480
LAYERS = 2
NAMES = ("w_gate", "w_up", "w_down")
SHAPES = {"w_gate": (LAYERS, D, FF), "w_up": (LAYERS, D, FF), "w_down": (LAYERS, FF, D)}


def bump(key, n, height):
    away = (jnp.arange(n, dtype=jnp.int32) - jax.random.randint(key, (), 0, n, jnp.int32)) % n
    return jnp.where(away < n // 8, height, 1.0)


def together(key, own, strength):
    shared = jax.random.normal(key, own.shape[1:], jnp.float32)
    return (own + strength * shared) * lax.rsqrt(1 + strength * strength)


def setup_inputs(seed: int = 0, part: int = 0) -> dict:
    kx, kdy, ka, kb, kz, kf, kh, kl, *keys = jax.random.split(jax.random.key(seed), 8 + 3 * len(NAMES))
    kx, kdy, ka, kb = (jax.random.fold_in(k, part) for k in (kx, kdy, ka, kb))
    kw, km, kv = (keys[i::3] for i in range(3))
    shape = (SEQUENCES, TOKENS, D)
    much_x, much_dy = jax.random.uniform(kz, (2,), jnp.float32, 0.0, 1.0)
    loud = 2.0 ** jax.random.uniform(jax.random.fold_in(kz, 1), (), jnp.float32, -1.0, 2.0)
    layers = 2.0 ** jax.random.uniform(kl, (LAYERS, 1, 1), jnp.float32, -1.0, 1.0)
    x = together(ka, jax.random.normal(kx, shape, jnp.float32), much_x) * bump(kf, D, 4.0)
    dy = together(kb, jax.random.normal(kdy, shape, jnp.float32), much_dy)
    drawn = {"x": x.astype(jnp.bfloat16), "dy": (loud * dy * (SEQUENCES * TOKENS) ** -0.5).astype(jnp.bfloat16)}
    for key, name in zip(kw, NAMES, strict=True):
        w = jax.random.normal(key, SHAPES[name], jnp.float32) * SHAPES[name][1] ** -0.5
        drawn[name] = (w * {"w_gate": 1.0, "w_up": bump(kh, FF, 4.0), "w_down": layers}[name]).astype(jnp.bfloat16)
    for key, name in zip(km, NAMES, strict=True):
        drawn[f"m_{name}"] = 0.1 * jax.random.normal(key, SHAPES[name], jnp.float32)
    for key, name in zip(kv, NAMES, strict=True):
        drawn[f"v_{name}"] = jax.random.uniform(key, SHAPES[name], jnp.float32, 0.005, 0.015)
    return drawn


def matmul(a, w):
    return jnp.dot(a, w, preferred_element_type=jnp.float32).astype(jnp.bfloat16)


def normed(h):
    wide = h.astype(jnp.float32)
    scale = lax.rsqrt(jnp.mean(wide**2, -1, keepdims=True) + 1e-6)
    return (wide * scale).astype(jnp.bfloat16)


def layer(h, w):
    a = normed(h)
    gate = jnp.dot(a, w["w_gate"], preferred_element_type=jnp.float32)
    up = jnp.dot(a, w["w_up"], preferred_element_type=jnp.float32)
    return h + matmul((jax.nn.silu(gate) * up).astype(jnp.bfloat16), w["w_down"])


def adamw(w, m, v, g):
    m = 0.9 * m + 0.1 * g
    v = 0.95 * v + 0.05 * g * g
    step = m * lax.rsqrt(v + 1e-8) + 0.1 * w
    return (w - 0.02 * step).astype(jnp.bfloat16), m, v


def stack(weights, h):
    return lax.scan(lambda h, w: (layer(h, w), None), h, weights)[0]


def reference(x, dy, w_gate, w_up, w_down, m_w_gate, m_w_up, m_w_down, v_w_gate, v_w_up, v_w_down):
    weights = dict(zip(NAMES, (w_gate, w_up, w_down), strict=True))

    def take(so_far, sequence):
        h, by_y = sequence
        _, back = jax.vjp(lambda w: stack(w, h), weights)
        return jax.tree.map(lambda total, term: total + term.astype(jnp.float32), so_far, back(by_y)[0]), None

    none_yet = {name: jnp.zeros(w.shape, jnp.float32) for name, w in weights.items()}
    by_weights, _ = lax.scan(take, none_yet, (x, dy))
    gradients = [by_weights[name].astype(jnp.bfloat16).astype(jnp.float32) for name in NAMES]
    new = [
        adamw(w.astype(jnp.float32), m, v, g)
        for w, m, v, g in zip((w_gate, w_up, w_down), (m_w_gate, m_w_up, m_w_down), (v_w_gate, v_w_up, v_w_down), gradients, strict=True)
    ]
    return tuple(one[which] for which in range(3) for one in new)
```

```python
import jax
import jax.numpy as jnp
from jax import lax
from jax.experimental import pallas as pl
from jax.experimental.pallas import tpu as pltpu
from jax.sharding import PartitionSpec as P

F32, BF16 = jnp.float32, jnp.bfloat16


def dot(a, w, dims=((1,), (0,))):
    return lax.dot_general(a, w, (dims, ((), ())), preferred_element_type=F32)


def scale_of(h):
    wide = h.astype(F32)
    return lax.rsqrt(jnp.mean(wide**2, -1, keepdims=True) + 1e-6)


def norm_back(by_a, h, scale):
    wide, by_a = h.astype(F32), by_a.astype(F32)
    by_scale = jnp.sum(by_a * wide, -1, keepdims=True)
    return by_a * scale - by_scale * scale**3 * wide / h.shape[-1]


def gates_back(by_hidden, gate, up):
    by = by_hidden.astype(F32)
    s = jax.nn.sigmoid(gate)
    return (by * up * (s * (1 + gate * (1 - s)))).astype(BF16), (by * (gate * s)).astype(BF16)


def adamw(w, m, v, g):
    m = 0.9 * m + 0.1 * g
    v = 0.95 * v + 0.05 * g * g
    step = m * lax.rsqrt(v + 1e-8) + 0.1 * w
    return (w - 0.02 * step).astype(BF16), m, v


def after(first, *rest):
    return lax.optimization_barrier((first, *rest))


MESH = pl.DeviceIdType.MESH
CORE, SIDE_Y, SIDE_X = 1, 2, 4
TILE = 640
ROWS = 256


def place():
    me = lax.axis_index("dp")
    bits = ((CORE, lax.rem(me, 2)), (SIDE_Y, lax.rem(me // 2, 2)), (SIDE_X, me // 4))

    def across(number, axes):
        for axis, bit in bits:
            if axes & axis:
                number = number + axis - 2 * axis * bit
        return number

    return me, across


def meet(me, across):
    barrier = pltpu.get_barrier_semaphore()
    for axis in (CORE, SIDE_Y, SIDE_X):
        pl.semaphore_signal(barrier, inc=1, device_id={"dp": across(me, axis)}, device_id_type=MESH)
    pl.semaphore_wait(barrier, 3)


class Gather:
    def __init__(self, me, across, shard, full, buffer, local, send, recv):
        self.me, self.across, self.shard, self.full, self.buffer = me, across, shard, full, buffer
        self.local, self.send, self.recv = local, send, recv
        self.rows = shard.shape[0]
        first = -(-self.rows // 32) * 16
        self.halves = ((0, first), (first, self.rows - first))
        self.sent = []

    def part(self, number, half):
        start, size = self.halves[half] if half is not None else (0, self.rows)
        return self.full.at[pl.ds(pl.multiple_of(number * self.rows + start, 16), size)]

    def remote(self, source, number, half, axis, slot):
        return pltpu.make_async_remote_copy(
            src_ref=source, dst_ref=self.part(number, half), send_sem=self.send.at[slot], recv_sem=self.recv.at[slot],
            device_id={"dp": self.across(self.me, axis)}, device_id_type=MESH,
        )

    def begin(self):
        pltpu.make_async_copy(self.shard, self.buffer, self.local.at[0]).start()
        for slot, half, axis in ((0, 0, SIDE_X), (2, 1, SIDE_Y), (1, 1, SIDE_X), (3, 0, SIDE_Y)):
            start, size = self.halves[half]
            copy = self.remote(self.shard.at[pl.ds(start, size)], self.me, half, axis, slot)
            copy.start()
            self.sent.append(copy)
        copy = self.remote(self.shard, self.me, None, CORE, 4)
        copy.start()
        self.sent.append(copy)

    def forward(self, number, half, axis, slot):
        copy = self.remote(self.part(number, half), number, half, axis, slot)
        copy.start()
        self.sent.append(copy)

    def got(self, number, half, slot):
        self.remote(self.part(number, half), number, half, CORE, slot).wait_recv()

    def relay(self):
        me, across = self.me, self.across
        pltpu.make_async_copy(self.shard, self.buffer, self.local.at[0]).wait()
        pltpu.make_async_copy(self.buffer, self.part(me, None), self.local.at[1]).start()
        self.got(across(me, SIDE_X), 0, 0)
        self.forward(across(me, SIDE_X), 0, SIDE_Y, 6)
        self.got(across(me, SIDE_Y), 1, 2)
        self.forward(across(me, SIDE_Y), 1, SIDE_X, 5)
        self.forward(across(me, SIDE_X), 0, CORE, 7)
        self.forward(across(me, SIDE_Y), 1, CORE, 8)

    def finish(self):
        me, across = self.me, self.across
        for axes, half, slot, on in ((SIDE_X, 1, 1, 9), (SIDE_Y, 0, 3, 10), (SIDE_X | SIDE_Y, 0, 6, 11), (SIDE_X | SIDE_Y, 1, 5, 12)):
            self.got(across(me, axes), half, slot)
            self.forward(across(me, axes), half, CORE, on)
        self.got(across(me, CORE), None, 4)
        for axes, half, slot in ((SIDE_X, 0, 7), (SIDE_Y, 1, 8), (SIDE_X, 1, 9), (SIDE_Y, 0, 10), (SIDE_X | SIDE_Y, 0, 11), (SIDE_X | SIDE_Y, 1, 12)):
            self.got(across(me, axes | CORE), half, slot)
        pltpu.make_async_copy(self.buffer, self.part(me, None), self.local.at[1]).wait()

    def close(self):
        for copy in self.sent:
            copy.wait_send()


def bring(source, target, sem):
    copy = pltpu.make_async_copy(source, target, sem)
    copy.start()
    copy.wait()


def forward_kernel(
    x, g, u, d, full_g0, full_u0, full_d0, full_g1, full_u1, full_d1, a0, gate0, up0, hidden0, h1, a1, gate1, up1, hidden1,
    states, down, small_a, small_b, wide_a, wide_b, local, send, recv, sem,
):
    me, across = place()
    order = (
        (g.at[0], full_g0, small_a), (u.at[0], full_u0, small_b), (d.at[0], full_d0, wide_a),
        (g.at[1], full_g1, small_a), (u.at[1], full_u1, small_b), (d.at[1], full_d1, wide_b),
    )
    gathers = [Gather(me, across, *refs, local.at[i], send.at[i], recv.at[i]) for i, refs in enumerate(order)]
    tokens, depth = states.shape
    wide = full_g0.shape[1]
    chunks = tokens // ROWS

    def rows(i):
        return pl.ds(pl.multiple_of(i * ROWS, ROWS), ROWS)

    def norm_of(value):
        value = value.astype(F32)
        return (value * lax.rsqrt(jnp.mean(value**2, -1, keepdims=True) + 1e-6)).astype(BF16)

    def gate_part(weight, gate, first, count):
        def body(w_tile, gate_tile):
            @pl.loop(0, chunks)
            def _(i):
                gate_tile[rows(i), :] = jnp.dot(states[rows(i), :], w_tile[...], preferred_element_type=F32)

        pltpu.emit_pipeline(
            body, grid=(count,),
            in_specs=[pl.BlockSpec((depth, TILE), lambda j: (0, j + first))],
            out_specs=[pl.BlockSpec((tokens, TILE), lambda j: (0, j + first))],
        )(weight, gate)

    def up_part(weight, gate, up, hidden, first, count):
        def body(w_tile, gate_tile, up_tile, hidden_tile):
            @pl.loop(0, chunks)
            def _(i):
                value = jnp.dot(states[rows(i), :], w_tile[...], preferred_element_type=F32)
                up_tile[rows(i), :] = value
                gate_value = gate_tile[rows(i), :]
                hidden_tile[rows(i), :] = (gate_value * jax.nn.sigmoid(gate_value) * value).astype(BF16)

        spec = pl.BlockSpec((tokens, TILE), lambda j: (0, j + first))
        pltpu.emit_pipeline(
            body, grid=(count,),
            in_specs=[pl.BlockSpec((depth, TILE), lambda j: (0, j + first)), spec],
            out_specs=[spec, spec],
        )(weight, gate, up, hidden)

    def down_part(first, count):
        def body(hidden_tile, x_tile, h_tile, a_tile):
            out = jnp.dot(hidden_tile[...], down[...], preferred_element_type=F32).astype(BF16)
            h = x_tile[...] + out
            h_tile[...] = h
            a_tile[...] = norm_of(h)

        spec = pl.BlockSpec((ROWS, depth), lambda i: (i + first, 0))
        pltpu.emit_pipeline(
            body, grid=(count,),
            in_specs=[pl.BlockSpec((ROWS, wide), lambda i: (i + first, 0)), spec],
            out_specs=[spec, spec],
        )(hidden0, x, h1, a1)

    meet(me, across)
    gathers[0].begin()
    bring(x.at[0] if x.ndim == 3 else x, states, sem)

    @pl.loop(0, chunks)
    def _(i):
        states[rows(i), :] = norm_of(states[rows(i), :])

    bring(states, a0, sem)

    def step(number, first_part, last_part):
        if first_part is not None:
            first_part()
        gathers[number].relay()
        if number + 1 < len(gathers):
            gathers[number + 1].begin()
        if last_part is not None:
            last_part()
        gathers[number].finish()

    tiles = wide // TILE
    most = (tiles + 1) // 2
    step(0, None, None)
    step(1, lambda: gate_part(full_g0, gate0, 0, most), lambda: gate_part(full_g0, gate0, most, tiles - most))
    step(2, lambda: up_part(full_u0, gate0, up0, hidden0, 0, most), lambda: up_part(full_u0, gate0, up0, hidden0, most, tiles - most))
    bring(full_d0, down, sem)
    step(3, lambda: down_part(0, chunks // 2), lambda: down_part(chunks // 2, chunks // 2))
    bring(a1, states, sem)
    step(4, lambda: gate_part(full_g1, gate1, 0, most), lambda: gate_part(full_g1, gate1, most, tiles - most))
    step(5, lambda: up_part(full_u1, gate1, up1, hidden1, 0, most), lambda: up_part(full_u1, gate1, up1, hidden1, most, tiles - most))
    for gather in gathers:
        gather.close()


def forward(x, w_gate, w_up, w_down):
    tokens, depth = x.shape
    wide = w_gate.shape[2]
    small, tall = (w_gate.shape[1], wide), (w_down.shape[1], depth)

    def array(shape, dtype=BF16):
        return jax.ShapeDtypeStruct(shape, dtype)

    into, out = array((depth, wide)), array((wide, depth))
    state, inner, inner32 = array((tokens, depth)), array((tokens, wide)), array((tokens, wide), F32)
    anywhere = pl.BlockSpec(memory_space=pl.ANY)
    shapes = [into, into, out, into, into, out, state, inner32, inner32, inner, state, state, inner32, inner32, inner]
    return pl.pallas_call(
        forward_kernel,
        name="forward",
        out_shape=shapes,
        in_specs=[anywhere] * 4,
        out_specs=[anywhere] * len(shapes),
        scratch_shapes=[
            pltpu.VMEM((tokens, depth), BF16), pltpu.VMEM((wide, depth), BF16),
            pltpu.VMEM(small, BF16), pltpu.VMEM(small, BF16), pltpu.VMEM(tall, BF16), pltpu.VMEM(tall, BF16),
            pltpu.SemaphoreType.DMA((6, 2)), pltpu.SemaphoreType.DMA((6, 13)), pltpu.SemaphoreType.DMA((6, 13)), pltpu.SemaphoreType.DMA,
        ],
        compiler_params=pltpu.CompilerParams(collective_id=0, has_side_effects=True, vmem_limit_bytes=66_000_000),
        cost_estimate=pl.CostEstimate(flops=10 * tokens * depth * wide, bytes_accessed=300_000_000, transcendentals=0),
    )(x, w_gate, w_up, w_down)


def solution(mesh):
    def scatter(g):
        return lax.psum_scatter(g, "dp", scatter_dimension=0, tiled=True)

    def step(x, dy, *arrays):
        weights, m, v = (arrays[i : i + 3] for i in (0, 3, 6))
        x, dy = x[0], dy[0]
        _, _, d0, g1, u1, d1, a0, gate0, up0, hidden0, h1, a1, gate1, up1, hidden1 = forward(x, *weights)
        s1 = scale_of(h1)

        rows = ((0,), (0,))
        by_d1 = dot(hidden1, dy, rows).astype(BF16)
        by_d1, dy_, gate1, up1 = after(by_d1, dy, gate1, up1)
        mine_d1 = scatter(by_d1)
        by_hidden1 = dot(dy_, d1, ((1,), (1,))).astype(BF16)
        by_gate1, by_up1 = after(*gates_back(by_hidden1, gate1, up1))
        by_g1 = dot(a1, by_gate1, rows).astype(BF16)
        by_g1, by_gate1, by_up1 = after(by_g1, by_gate1, by_up1)
        mine_g1 = scatter(by_g1)
        by_u1 = dot(a1, by_up1, rows).astype(BF16)
        by_u1, by_gate1, by_up1 = after(by_u1, by_gate1, by_up1)
        mine_u1 = scatter(by_u1)
        by_a1 = dot(by_gate1, g1, ((1,), (1,))).astype(BF16) + dot(by_up1, u1, ((1,), (1,))).astype(BF16)
        by_h1 = norm_back(by_a1, h1, s1).astype(BF16) + dy
        (by_h1,) = after(by_h1)
        by_d0 = dot(hidden0, by_h1, rows).astype(BF16)
        by_d0, by_h1, gate0, up0 = after(by_d0, by_h1, gate0, up0)
        mine_d0 = scatter(by_d0)
        by_hidden0 = dot(by_h1, d0, ((1,), (1,))).astype(BF16)
        by_gate0, by_up0 = after(*gates_back(by_hidden0, gate0, up0))
        by_g0 = dot(a0, by_gate0, rows).astype(BF16)
        by_g0, by_up0 = after(by_g0, by_up0)
        mine_g0 = scatter(by_g0)
        mine_u0 = scatter(dot(a0, by_up0, rows).astype(BF16))

        gradients = [jnp.stack(pair).astype(F32) for pair in ((mine_g0, mine_g1), (mine_u0, mine_u1), (mine_d0, mine_d1))]
        new = [adamw(w.astype(F32), m, v, g) for w, m, v, g in zip(weights, m, v, gradients, strict=True)]
        return tuple(one[which] for which in range(3) for one in new)

    states, cut = P(("rep", "dp"), None, None), P(None, "dp", None)
    return jax.shard_map(
        step,
        mesh=mesh,
        in_specs=(states, states) + (cut,) * 9,
        out_specs=(P("rep", "dp", None),) * 9,
        check_vma=False,
    )
```

```python
import jax
import jax.numpy as jnp
from jax import lax
from jax.experimental import pallas as pl
from jax.experimental.pallas import tpu as pltpu
from jax.sharding import PartitionSpec as P

F32, BF16 = jnp.float32, jnp.bfloat16


def dot(a, w, dims=((1,), (0,))):
    return lax.dot_general(a, w, (dims, ((), ())), preferred_element_type=F32)


def scale_of(h):
    wide = h.astype(F32)
    return lax.rsqrt(jnp.mean(wide**2, -1, keepdims=True) + 1e-6)


def norm_back(by_a, h, scale):
    wide, by_a = h.astype(F32), by_a.astype(F32)
    by_scale = jnp.sum(by_a * wide, -1, keepdims=True)
    return by_a * scale - by_scale * scale**3 * wide / h.shape[-1]


def gates_back(by_hidden, gate, up):
    by = by_hidden.astype(F32)
    s = jax.nn.sigmoid(gate)
    return (by * up * (s * (1 + gate * (1 - s)))).astype(BF16), (by * (gate * s)).astype(BF16)


def adamw(w, m, v, g):
    m = 0.9 * m + 0.1 * g
    v = 0.95 * v + 0.05 * g * g
    step = m * lax.rsqrt(v + 1e-8) + 0.1 * w
    return (w - 0.02 * step).astype(BF16), m, v


def after(first, *rest):
    return lax.optimization_barrier((first, *rest))


MESH = pl.DeviceIdType.MESH
CORE, SIDE_Y, SIDE_X = 1, 2, 4
TILE = 640
ROWS = 256
TALL = 1024


def place():
    me = lax.axis_index("dp")
    bits = ((CORE, lax.rem(me, 2)), (SIDE_Y, lax.rem(me // 2, 2)), (SIDE_X, me // 4))

    def across(number, axes):
        for axis, bit in bits:
            if axes & axis:
                number = number + axis - 2 * axis * bit
        return number

    return me, across


def meet(me, across):
    barrier = pltpu.get_barrier_semaphore()
    for axis in (CORE, SIDE_Y, SIDE_X):
        pl.semaphore_signal(barrier, inc=1, device_id={"dp": across(me, axis)}, device_id_type=MESH)
    pl.semaphore_wait(barrier, 3)


class Gather:
    def __init__(self, me, across, shard, full, buffer, local, send, recv):
        self.me, self.across, self.shard, self.full, self.buffer = me, across, shard, full, buffer
        self.local, self.send, self.recv = local, send, recv
        self.rows = shard.shape[0]
        first = -(-self.rows // 32) * 16
        self.halves = ((0, first), (first, self.rows - first))
        self.sent = []

    def part(self, number, half):
        start, size = self.halves[half] if half is not None else (0, self.rows)
        return self.full.at[pl.ds(pl.multiple_of(number * self.rows + start, 16), size)]

    def remote(self, source, number, half, axis, slot):
        return pltpu.make_async_remote_copy(
            src_ref=source, dst_ref=self.part(number, half), send_sem=self.send.at[slot], recv_sem=self.recv.at[slot],
            device_id={"dp": self.across(self.me, axis)}, device_id_type=MESH,
        )

    def begin(self):
        pltpu.make_async_copy(self.shard, self.buffer, self.local.at[0]).start()
        for slot, half, axis in ((0, 0, SIDE_X), (2, 1, SIDE_Y), (1, 1, SIDE_X), (3, 0, SIDE_Y)):
            start, size = self.halves[half]
            copy = self.remote(self.shard.at[pl.ds(start, size)], self.me, half, axis, slot)
            copy.start()
            self.sent.append(copy)
        copy = self.remote(self.shard, self.me, None, CORE, 4)
        copy.start()
        self.sent.append(copy)

    def forward(self, number, half, axis, slot):
        copy = self.remote(self.part(number, half), number, half, axis, slot)
        copy.start()
        self.sent.append(copy)

    def got(self, number, half, slot):
        self.remote(self.part(number, half), number, half, CORE, slot).wait_recv()

    def relay(self):
        me, across = self.me, self.across
        pltpu.make_async_copy(self.shard, self.buffer, self.local.at[0]).wait()
        pltpu.make_async_copy(self.buffer, self.part(me, None), self.local.at[1]).start()
        self.got(across(me, SIDE_X), 0, 0)
        self.forward(across(me, SIDE_X), 0, SIDE_Y, 6)
        self.got(across(me, SIDE_Y), 1, 2)
        self.forward(across(me, SIDE_Y), 1, SIDE_X, 5)
        self.forward(across(me, SIDE_X), 0, CORE, 7)
        self.forward(across(me, SIDE_Y), 1, CORE, 8)

    def finish(self):
        me, across = self.me, self.across
        for axes, half, slot, on in ((SIDE_X, 1, 1, 9), (SIDE_Y, 0, 3, 10), (SIDE_X | SIDE_Y, 0, 6, 11), (SIDE_X | SIDE_Y, 1, 5, 12)):
            self.got(across(me, axes), half, slot)
            self.forward(across(me, axes), half, CORE, on)
        self.got(across(me, CORE), None, 4)
        for axes, half, slot in ((SIDE_X, 0, 7), (SIDE_Y, 1, 8), (SIDE_X, 1, 9), (SIDE_Y, 0, 10), (SIDE_X | SIDE_Y, 0, 11), (SIDE_X | SIDE_Y, 1, 12)):
            self.got(across(me, axes | CORE), half, slot)
        pltpu.make_async_copy(self.buffer, self.part(me, None), self.local.at[1]).wait()

    def close(self):
        for copy in self.sent:
            copy.wait_send()


def bring(source, target, sem):
    copy = pltpu.make_async_copy(source, target, sem)
    copy.start()
    copy.wait()


def forward_kernel(
    x, g, u, d, full_g0, full_u0, full_d0, full_g1, full_u1, full_d1, a0, gate0, up0, hidden0, h1, a1, gate1, up1, hidden1,
    states, down, small_a, small_b, wide_a, wide_b, local, send, recv, sem,
):
    me, across = place()
    order = (
        (g.at[0], full_g0, small_a), (u.at[0], full_u0, small_b), (d.at[0], full_d0, wide_a),
        (g.at[1], full_g1, small_a), (u.at[1], full_u1, small_b), (d.at[1], full_d1, wide_b),
    )
    gathers = [Gather(me, across, *refs, local.at[i], send.at[i], recv.at[i]) for i, refs in enumerate(order)]
    tokens, depth = states.shape
    wide = full_g0.shape[1]
    chunks = tokens // ROWS

    def rows(i):
        return pl.ds(pl.multiple_of(i * ROWS, ROWS), ROWS)

    def tall(i):
        return pl.ds(pl.multiple_of(i * TALL, TALL), TALL)

    def norm_of(value):
        value = value.astype(F32)
        return (value * lax.rsqrt(jnp.mean(value**2, -1, keepdims=True) + 1e-6)).astype(BF16)

    def gate_part(weight, gate, first, count):
        def body(w_tile, gate_tile):
            @pl.loop(0, tokens // TALL)
            def _(i):
                gate_tile[tall(i), :] = jnp.dot(states[tall(i), :], w_tile[...], preferred_element_type=F32)

        pltpu.emit_pipeline(
            body, grid=(count,),
            in_specs=[pl.BlockSpec((depth, TILE), lambda j: (0, j + first))],
            out_specs=[pl.BlockSpec((tokens, TILE), lambda j: (0, j + first))],
        )(weight, gate)

    def up_part(weight, gate, up, hidden, first, count):
        def body(w_tile, gate_tile, up_tile, hidden_tile):
            @pl.loop(0, tokens // TALL)
            def _(i):
                value = jnp.dot(states[tall(i), :], w_tile[...], preferred_element_type=F32)
                up_tile[tall(i), :] = value
                gate_value = gate_tile[tall(i), :]
                hidden_tile[tall(i), :] = (gate_value * jax.nn.sigmoid(gate_value) * value).astype(BF16)

        spec = pl.BlockSpec((tokens, TILE), lambda j: (0, j + first))
        pltpu.emit_pipeline(
            body, grid=(count,),
            in_specs=[pl.BlockSpec((depth, TILE), lambda j: (0, j + first)), spec],
            out_specs=[spec, spec],
        )(weight, gate, up, hidden)

    def down_part(first, count):
        def body(hidden_tile, x_tile, h_tile, a_tile):
            out = jnp.dot(hidden_tile[...], down[...], preferred_element_type=F32).astype(BF16)
            h = x_tile[...] + out
            h_tile[...] = h
            a_tile[...] = norm_of(h)

        spec = pl.BlockSpec((ROWS, depth), lambda i: (i + first, 0))
        pltpu.emit_pipeline(
            body, grid=(count,),
            in_specs=[pl.BlockSpec((ROWS, wide), lambda i: (i + first, 0)), spec],
            out_specs=[spec, spec],
        )(hidden0, x, h1, a1)

    meet(me, across)
    gathers[0].begin()
    bring(x.at[0] if x.ndim == 3 else x, states, sem)

    @pl.loop(0, chunks)
    def _(i):
        states[rows(i), :] = norm_of(states[rows(i), :])

    bring(states, a0, sem)

    def step(number, first_part, last_part):
        if first_part is not None:
            first_part()
        gathers[number].relay()
        if number + 1 < len(gathers):
            gathers[number + 1].begin()
        if last_part is not None:
            last_part()
        gathers[number].finish()

    tiles = wide // TILE
    most = (tiles + 1) // 2
    step(0, None, None)
    step(1, lambda: gate_part(full_g0, gate0, 0, most), lambda: gate_part(full_g0, gate0, most, tiles - most))
    step(2, lambda: up_part(full_u0, gate0, up0, hidden0, 0, most), lambda: up_part(full_u0, gate0, up0, hidden0, most, tiles - most))
    bring(full_d0, down, sem)
    step(3, lambda: down_part(0, chunks // 2), lambda: down_part(chunks // 2, chunks // 2))
    bring(a1, states, sem)
    step(4, lambda: gate_part(full_g1, gate1, 0, most), lambda: gate_part(full_g1, gate1, most, tiles - most))
    step(5, lambda: up_part(full_u1, gate1, up1, hidden1, 0, most), lambda: up_part(full_u1, gate1, up1, hidden1, most, tiles - most))
    for gather in gathers:
        gather.close()


def forward(x, w_gate, w_up, w_down):
    tokens, depth = x.shape
    wide = w_gate.shape[2]
    small, tall = (w_gate.shape[1], wide), (w_down.shape[1], depth)

    def array(shape, dtype=BF16):
        return jax.ShapeDtypeStruct(shape, dtype)

    into, out = array((depth, wide)), array((wide, depth))
    state, inner, inner32 = array((tokens, depth)), array((tokens, wide)), array((tokens, wide), F32)
    anywhere = pl.BlockSpec(memory_space=pl.ANY)
    shapes = [into, into, out, into, into, out, state, inner32, inner32, inner, state, state, inner32, inner32, inner]
    return pl.pallas_call(
        forward_kernel,
        name="forward",
        out_shape=shapes,
        in_specs=[anywhere] * 4,
        out_specs=[anywhere] * len(shapes),
        scratch_shapes=[
            pltpu.VMEM((tokens, depth), BF16), pltpu.VMEM((wide, depth), BF16),
            pltpu.VMEM(small, BF16), pltpu.VMEM(small, BF16), pltpu.VMEM(tall, BF16), pltpu.VMEM(tall, BF16),
            pltpu.SemaphoreType.DMA((6, 2)), pltpu.SemaphoreType.DMA((6, 13)), pltpu.SemaphoreType.DMA((6, 13)), pltpu.SemaphoreType.DMA,
        ],
        compiler_params=pltpu.CompilerParams(collective_id=0, has_side_effects=True, vmem_limit_bytes=66_000_000),
        cost_estimate=pl.CostEstimate(flops=10 * tokens * depth * wide, bytes_accessed=300_000_000, transcendentals=0),
    )(x, w_gate, w_up, w_down)


HELD, SLOTS = 6, 4


def sums_kernel(a, by_gate, by_up, mine_g, mine_u, states, tiles, terms, out, core_out, core_in, far_out, far_in, near_out, near_in, local, core_s, core_r, far_s, far_r, near_s, near_r):
    me, across = place()
    _, depth = states.shape
    block = depth // 8
    half = block // 2
    count = by_gate.shape[1] // TILE
    sources, outs = (by_gate, by_up), (mine_g, mine_u)

    def columns(j):
        return pl.ds(pl.multiple_of(j * TILE, 128), TILE)

    def load(p, j):
        return pltpu.make_async_copy(sources[p].at[:, columns(j)], tiles.at[p], local.at[p])

    def rows(number, start=0, size=block):
        return pl.ds(pl.multiple_of(number * block + start, 16), size)

    def core_copy(slot):
        return pltpu.make_async_remote_copy(
            src_ref=core_out.at[slot], dst_ref=core_in.at[slot], send_sem=core_s.at[slot], recv_sem=core_r.at[slot],
            device_id={"dp": across(me, CORE)}, device_id_type=MESH,
        )

    def side_copy(source, target, sent, come, slot, side):
        return pltpu.make_async_remote_copy(
            src_ref=source.at[slot, side], dst_ref=target.at[slot, side], send_sem=sent.at[slot, side], recv_sem=come.at[slot, side],
            device_id={"dp": across(me, (SIDE_X, SIDE_Y)[side])}, device_id_type=MESH,
        )

    def far_copy(slot, side):
        return side_copy(far_out, far_in, far_s, far_r, slot, side)

    def near_copy(slot, side):
        return side_copy(near_out, near_in, near_s, near_r, slot, side)

    blocks = (0, SIDE_X, SIDE_Y, SIDE_X | SIDE_Y)

    def multiply(t, p, j):
        load(p, j).wait()
        held = lax.rem(t, HELD)

        @pl.loop(0, depth // TILE)
        def _(i):
            part = pl.ds(pl.multiple_of(i * TILE, TILE), TILE)
            terms[held, part, :] = lax.dot_general(
                states[:, part], tiles[p], (((0,), (0,)), ((), ())), preferred_element_type=F32
            )

        @pl.when(j + 1 < count)
        def _():
            load(p, j + 1).start()

    def to_core(t):
        slot, held = lax.rem(t, SLOTS), lax.rem(t, HELD)

        @pl.when(t >= SLOTS)
        def _():
            core_copy(slot).wait_send()

        for i, axes in enumerate(blocks):
            core_out[slot, i] = terms[held, rows(across(me, axes | CORE)), :].astype(BF16)
        core_copy(slot).start()

    def to_far(t):
        slot, held = lax.rem(t, SLOTS), lax.rem(t, HELD)
        core_copy(slot).wait_recv()

        @pl.when(t >= SLOTS)
        def _():
            far_copy(slot, 0).wait_send()
            far_copy(slot, 1).wait_send()

        last = terms[held, rows(across(me, blocks[3])), :] + core_in[slot, 3].astype(F32)
        for side in (0, 1):
            far_out[slot, side] = last[side * half : (side + 1) * half].astype(BF16)
            far_copy(slot, side).start()
        for i, axes in enumerate(blocks[:3]):
            terms[held, rows(across(me, axes)), :] += core_in[slot, i].astype(F32)

    def to_near(t):
        slot, held = lax.rem(t, SLOTS), lax.rem(t, HELD)
        far_copy(slot, 0).wait_recv()
        far_copy(slot, 1).wait_recv()

        @pl.when(t >= SLOTS)
        def _():
            near_copy(slot, 0).wait_send()
            near_copy(slot, 1).wait_send()

        for side in (0, 1):
            number = across(me, (SIDE_X, SIDE_Y)[side])
            extra, plain = (half, 0) if side == 0 else (0, half)
            near_out[slot, side, pl.ds(plain, half)] = terms[held, rows(number, plain, half), :].astype(BF16)
            near_out[slot, side, pl.ds(extra, half)] = (
                terms[held, rows(number, extra, half), :] + far_in[slot, 1 - side].astype(F32)
            ).astype(BF16)
        near_copy(slot, 0).start()
        near_copy(slot, 1).start()

    def to_out(t, p, j):
        slot, held = lax.rem(t, SLOTS), lax.rem(t, HELD)
        near_copy(slot, 0).wait_recv()
        near_copy(slot, 1).wait_recv()
        total = terms[held, rows(me), :] + near_in[slot, 0].astype(F32) + near_in[slot, 1].astype(F32)
        out[p, :, columns(j)] = total.astype(BF16)

    meet(me, across)
    load(0, 0).start()
    load(1, 0).start()
    bring(a, states, local.at[2])

    @pl.loop(0, count + 3)
    def _(j):
        for p in (0, 1):
            t = 2 * j + p

            @pl.when(j < count)
            def _():
                multiply(t, p, j)

            def stage(lag, run):
                q = (p - lag) % 2
                behind = (lag - p + q) // 2

                @pl.when((j >= behind) & (j - behind < count))
                def _():
                    run(t - lag, q, j - behind)

            stage(5, to_out)
            stage(3, lambda t, q, j: to_near(t))
            stage(1, lambda t, q, j: to_far(t))

            @pl.when(j < count)
            def _():
                to_core(t)

    for slot in range(SLOTS):
        core_copy(slot).wait_send()
        for side in (0, 1):
            far_copy(slot, side).wait_send()
            near_copy(slot, side).wait_send()
    for p in (0, 1):
        bring(out.at[p], outs[p], local.at[2])


def sums(a, by_gate, by_up):
    tokens, depth = a.shape
    wide = by_gate.shape[1]
    block = depth // 8
    anywhere = pl.BlockSpec(memory_space=pl.ANY)
    return pl.pallas_call(
        sums_kernel,
        name="sums",
        out_shape=[jax.ShapeDtypeStruct((block, wide), BF16)] * 2,
        in_specs=[anywhere] * 3,
        out_specs=[anywhere] * 2,
        scratch_shapes=[
            pltpu.VMEM((tokens, depth), BF16), pltpu.VMEM((2, tokens, TILE), BF16), pltpu.VMEM((HELD, depth, TILE), F32),
            pltpu.VMEM((2, block, wide), BF16),
            pltpu.VMEM((SLOTS, 4, block, TILE), BF16), pltpu.VMEM((SLOTS, 4, block, TILE), BF16),
            pltpu.VMEM((SLOTS, 2, block // 2, TILE), BF16), pltpu.VMEM((SLOTS, 2, block // 2, TILE), BF16),
            pltpu.VMEM((SLOTS, 2, block, TILE), BF16), pltpu.VMEM((SLOTS, 2, block, TILE), BF16),
            pltpu.SemaphoreType.DMA((3,)),
            pltpu.SemaphoreType.DMA((SLOTS,)), pltpu.SemaphoreType.DMA((SLOTS,)),
            pltpu.SemaphoreType.DMA((SLOTS, 2)), pltpu.SemaphoreType.DMA((SLOTS, 2)),
            pltpu.SemaphoreType.DMA((SLOTS, 2)), pltpu.SemaphoreType.DMA((SLOTS, 2)),
        ],
        compiler_params=pltpu.CompilerParams(collective_id=1, has_side_effects=True, vmem_limit_bytes=66_000_000),
        cost_estimate=pl.CostEstimate(flops=4 * tokens * depth * wide, bytes_accessed=60_000_000, transcendentals=0),
    )(a, by_gate, by_up)


def solution(mesh):
    def scatter(g):
        return lax.psum_scatter(g, "dp", scatter_dimension=0, tiled=True)

    def step(x, dy, *arrays):
        weights, m, v = (arrays[i : i + 3] for i in (0, 3, 6))
        x, dy = x[0], dy[0]
        _, _, d0, g1, u1, d1, a0, gate0, up0, hidden0, h1, a1, gate1, up1, hidden1 = forward(x, *weights)
        s1 = scale_of(h1)

        rows = ((0,), (0,))
        by_d1 = dot(hidden1, dy, rows).astype(BF16)
        by_d1, dy_, gate1, up1 = after(by_d1, dy, gate1, up1)
        mine_d1 = scatter(by_d1)
        by_hidden1 = dot(dy_, d1, ((1,), (1,))).astype(BF16)
        by_gate1, by_up1 = after(*gates_back(by_hidden1, gate1, up1))
        by_g1 = dot(a1, by_gate1, rows).astype(BF16)
        by_g1, by_gate1, by_up1 = after(by_g1, by_gate1, by_up1)
        mine_g1 = scatter(by_g1)
        by_u1 = dot(a1, by_up1, rows).astype(BF16)
        by_u1, by_gate1, by_up1 = after(by_u1, by_gate1, by_up1)
        mine_u1 = scatter(by_u1)
        by_a1 = dot(by_gate1, g1, ((1,), (1,))).astype(BF16) + dot(by_up1, u1, ((1,), (1,))).astype(BF16)
        by_h1 = norm_back(by_a1, h1, s1).astype(BF16) + dy
        (by_h1,) = after(by_h1)
        by_d0 = dot(hidden0, by_h1, rows).astype(BF16)
        by_d0, by_h1, gate0, up0 = after(by_d0, by_h1, gate0, up0)
        mine_d0 = scatter(by_d0)
        by_hidden0 = dot(by_h1, d0, ((1,), (1,))).astype(BF16)
        by_gate0, by_up0 = after(*gates_back(by_hidden0, gate0, up0))
        mine_g0, mine_u0 = sums(a0, by_gate0, by_up0)

        gradients = [jnp.stack(pair).astype(F32) for pair in ((mine_g0, mine_g1), (mine_u0, mine_u1), (mine_d0, mine_d1))]
        new = [adamw(w.astype(F32), m, v, g) for w, m, v, g in zip(weights, m, v, gradients, strict=True)]
        return tuple(one[which] for which in range(3) for one in new)

    states, cut = P(("rep", "dp"), None, None), P(None, "dp", None)
    return jax.shard_map(
        step,
        mesh=mesh,
        in_specs=(states, states) + (cut,) * 9,
        out_specs=(P("rep", "dp", None),) * 9,
        check_vma=False,
    )
```

```python
import jax
import jax.numpy as jnp
from jax import lax
from jax.experimental import pallas as pl
from jax.experimental.pallas import tpu as pltpu
from jax.sharding import PartitionSpec as P

F32, BF16 = jnp.float32, jnp.bfloat16


def dot(a, w, dims=((1,), (0,))):
    return lax.dot_general(a, w, (dims, ((), ())), preferred_element_type=F32)


def scale_of(h):
    wide = h.astype(F32)
    return lax.rsqrt(jnp.mean(wide**2, -1, keepdims=True) + 1e-6)


def norm_back(by_a, h, scale):
    wide, by_a = h.astype(F32), by_a.astype(F32)
    by_scale = jnp.sum(by_a * wide, -1, keepdims=True)
    return by_a * scale - by_scale * scale**3 * wide / h.shape[-1]


def gates_back(by_hidden, gate, up):
    by = by_hidden.astype(F32)
    s = jax.nn.sigmoid(gate)
    return (by * up * (s * (1 + gate * (1 - s)))).astype(BF16), (by * (gate * s)).astype(BF16)


def adamw(w, m, v, g):
    m = 0.9 * m + 0.1 * g
    v = 0.95 * v + 0.05 * g * g
    step = m * lax.rsqrt(v + 1e-8) + 0.1 * w
    return (w - 0.02 * step).astype(BF16), m, v


def after(first, *rest):
    return lax.optimization_barrier((first, *rest))


MESH = pl.DeviceIdType.MESH
CORE, SIDE_Y, SIDE_X = 1, 2, 4
TILE = 640
ROWS = 256
TALL = 1024


def place():
    me = lax.axis_index("dp")
    bits = ((CORE, lax.rem(me, 2)), (SIDE_Y, lax.rem(me // 2, 2)), (SIDE_X, me // 4))

    def across(number, axes):
        for axis, bit in bits:
            if axes & axis:
                number = number + axis - 2 * axis * bit
        return number

    return me, across


def meet(me, across):
    barrier = pltpu.get_barrier_semaphore()
    for axis in (CORE, SIDE_Y, SIDE_X):
        pl.semaphore_signal(barrier, inc=1, device_id={"dp": across(me, axis)}, device_id_type=MESH)
    pl.semaphore_wait(barrier, 3)


class Gather:
    def __init__(self, me, across, shard, full, buffer, local, send, recv):
        self.me, self.across, self.shard, self.full, self.buffer = me, across, shard, full, buffer
        self.local, self.send, self.recv = local, send, recv
        self.rows = shard.shape[0]
        first = -(-self.rows // 32) * 16
        self.halves = ((0, first), (first, self.rows - first))

    def part(self, number, half):
        start, size = self.halves[half] if half is not None else (0, self.rows)
        return self.full.at[pl.ds(pl.multiple_of(number * self.rows + start, 16), size)]

    def remote(self, source, number, half, axis, slot):
        return pltpu.make_async_remote_copy(
            src_ref=source, dst_ref=self.part(number, half), send_sem=self.send.at[slot], recv_sem=self.recv.at[slot],
            device_id={"dp": self.across(self.me, axis)}, device_id_type=MESH,
        )

    def begin(self):
        pltpu.make_async_copy(self.shard, self.buffer, self.local.at[0]).start()
        for slot, half, axis in ((0, 0, SIDE_X), (2, 1, SIDE_Y), (1, 1, SIDE_X), (3, 0, SIDE_Y)):
            start, size = self.halves[half]
            self.remote(self.shard.at[pl.ds(start, size)], self.me, half, axis, slot).start()
        self.remote(self.shard, self.me, None, CORE, 4).start()

    def forward(self, number, half, axis, slot):
        self.remote(self.part(number, half), number, half, axis, slot).start()

    def got(self, number, half, slot):
        self.remote(self.part(number, half), number, half, CORE, slot).wait_recv()

    def relay(self):
        me, across = self.me, self.across
        pltpu.make_async_copy(self.shard, self.buffer, self.local.at[0]).wait()
        pltpu.make_async_copy(self.buffer, self.part(me, None), self.local.at[1]).start()
        self.got(across(me, SIDE_X), 0, 0)
        self.forward(across(me, SIDE_X), 0, SIDE_Y, 6)
        self.got(across(me, SIDE_Y), 1, 2)
        self.forward(across(me, SIDE_Y), 1, SIDE_X, 5)
        self.forward(across(me, SIDE_X), 0, CORE, 7)
        self.forward(across(me, SIDE_Y), 1, CORE, 8)

    def finish(self):
        me, across = self.me, self.across
        for axes, half, slot, on in ((SIDE_X, 1, 1, 9), (SIDE_Y, 0, 3, 10), (SIDE_X | SIDE_Y, 0, 6, 11), (SIDE_X | SIDE_Y, 1, 5, 12)):
            self.got(across(me, axes), half, slot)
            self.forward(across(me, axes), half, CORE, on)
        self.got(across(me, CORE), None, 4)
        for axes, half, slot in ((SIDE_X, 0, 7), (SIDE_Y, 1, 8), (SIDE_X, 1, 9), (SIDE_Y, 0, 10), (SIDE_X | SIDE_Y, 0, 11), (SIDE_X | SIDE_Y, 1, 12)):
            self.got(across(me, axes | CORE), half, slot)
        pltpu.make_async_copy(self.buffer, self.part(me, None), self.local.at[1]).wait()

    def close(self):
        for slot, half in enumerate((0, 1, 1, 0, None, 1, 0, 0, 1, 1, 0, 0, 1)):
            self.remote(self.part(self.me, half), self.me, half, CORE, slot).wait_send()


def bring(source, target, sem):
    copy = pltpu.make_async_copy(source, target, sem)
    copy.start()
    copy.wait()


def forward_kernel(
    x, g, u, d, full_g0, full_u0, full_d0, full_g1, full_u1, full_d1, a0, gate0, up0, hidden0, h1, a1, gate1, up1, hidden1,
    states, down, small_a, small_b, wide_a, wide_b, local, send, recv, sem,
):
    me, across = place()
    order = (
        (g.at[0], full_g0, small_a), (u.at[0], full_u0, small_b), (d.at[0], full_d0, wide_a),
        (g.at[1], full_g1, small_a), (u.at[1], full_u1, small_b), (d.at[1], full_d1, wide_b),
    )
    gathers = [Gather(me, across, *refs, local.at[i], send.at[i], recv.at[i]) for i, refs in enumerate(order)]
    tokens, depth = states.shape
    wide = full_g0.shape[1]
    chunks = tokens // ROWS

    def rows(i):
        return pl.ds(pl.multiple_of(i * ROWS, ROWS), ROWS)

    def tall(i):
        return pl.ds(pl.multiple_of(i * TALL, TALL), TALL)

    def norm_of(value):
        value = value.astype(F32)
        return (value * lax.rsqrt(jnp.mean(value**2, -1, keepdims=True) + 1e-6)).astype(BF16)

    def midway(number):
        gathers[number].relay()
        if number + 1 < len(gathers):
            gathers[number + 1].begin()

    def midway_at(number, tile):
        @pl.when(pl.program_id(0) == tile)
        def _():
            midway(number)

    def gate_stage(number, weight, gate):
        def body(w_tile, gate_tile):
            midway_at(number, 3)

            @pl.loop(0, tokens // TALL)
            def _(i):
                gate_tile[tall(i), :] = jnp.dot(states[tall(i), :], w_tile[...], preferred_element_type=F32)

        spec = pl.BlockSpec((tokens, TILE), lambda j: (0, j))
        pltpu.emit_pipeline(body, grid=(wide // TILE,), in_specs=[pl.BlockSpec((depth, TILE), lambda j: (0, j))], out_specs=[spec])(weight, gate)
        gathers[number].finish()

    def up_stage(number, weight, gate, up, hidden):
        def body(w_tile, gate_tile, up_tile, hidden_tile):
            midway_at(number, 3)

            @pl.loop(0, tokens // TALL)
            def _(i):
                value = jnp.dot(states[tall(i), :], w_tile[...], preferred_element_type=F32)
                up_tile[tall(i), :] = value
                gate_value = gate_tile[tall(i), :]
                hidden_tile[tall(i), :] = (gate_value * jax.nn.sigmoid(gate_value) * value).astype(BF16)

        spec = pl.BlockSpec((tokens, TILE), lambda j: (0, j))
        pltpu.emit_pipeline(
            body, grid=(wide // TILE,), in_specs=[pl.BlockSpec((depth, TILE), lambda j: (0, j)), spec], out_specs=[spec, spec]
        )(weight, gate, up, hidden)
        gathers[number].finish()

    def down_stage(number):
        def body(hidden_tile, x_tile, h_tile, a_tile):
            midway_at(number, 5)
            out = jnp.dot(hidden_tile[...], down[...], preferred_element_type=F32).astype(BF16)
            h = x_tile[...] + out
            h_tile[...] = h
            a_tile[...] = norm_of(h)

        spec = pl.BlockSpec((ROWS, depth), lambda i: (i, 0))
        pltpu.emit_pipeline(
            body, grid=(chunks,), in_specs=[pl.BlockSpec((ROWS, wide), lambda i: (i, 0)), spec], out_specs=[spec, spec]
        )(hidden0, x, h1, a1)
        gathers[number].finish()

    meet(me, across)
    gathers[0].begin()
    bring(x.at[0] if x.ndim == 3 else x, states, sem)

    @pl.loop(0, chunks)
    def _(i):
        states[rows(i), :] = norm_of(states[rows(i), :])

    bring(states, a0, sem)

    midway(0)
    gathers[0].finish()
    gate_stage(1, full_g0, gate0)
    up_stage(2, full_u0, gate0, up0, hidden0)
    bring(full_d0, down, sem)
    down_stage(3)
    bring(a1, states, sem)
    gate_stage(4, full_g1, gate1)
    up_stage(5, full_u1, gate1, up1, hidden1)
    for gather in gathers:
        gather.close()


def forward(x, w_gate, w_up, w_down):
    tokens, depth = x.shape
    wide = w_gate.shape[2]
    small, tall = (w_gate.shape[1], wide), (w_down.shape[1], depth)

    def array(shape, dtype=BF16):
        return jax.ShapeDtypeStruct(shape, dtype)

    into, out = array((depth, wide)), array((wide, depth))
    state, inner, inner32 = array((tokens, depth)), array((tokens, wide)), array((tokens, wide), F32)
    anywhere = pl.BlockSpec(memory_space=pl.ANY)
    shapes = [into, into, out, into, into, out, state, inner32, inner32, inner, state, state, inner32, inner32, inner]
    return pl.pallas_call(
        forward_kernel,
        name="forward",
        out_shape=shapes,
        in_specs=[anywhere] * 4,
        out_specs=[anywhere] * len(shapes),
        scratch_shapes=[
            pltpu.VMEM((tokens, depth), BF16), pltpu.VMEM((wide, depth), BF16),
            pltpu.VMEM(small, BF16), pltpu.VMEM(small, BF16), pltpu.VMEM(tall, BF16), pltpu.VMEM(tall, BF16),
            pltpu.SemaphoreType.DMA((6, 2)), pltpu.SemaphoreType.DMA((6, 13)), pltpu.SemaphoreType.DMA((6, 13)), pltpu.SemaphoreType.DMA,
        ],
        compiler_params=pltpu.CompilerParams(collective_id=0, has_side_effects=True, vmem_limit_bytes=67_000_000),
        cost_estimate=pl.CostEstimate(flops=10 * tokens * depth * wide, bytes_accessed=300_000_000, transcendentals=0),
    )(x, w_gate, w_up, w_down)


HELD, SLOTS = 6, 4
SHORT = 512
CUT = 640


def sums_kernel(
    a, by_out, down, gate, up, mine_g, mine_u, states, outer, downs, inner, tiles, terms, out,
    core_out, core_in, far_out, far_in, near_out, near_in, local, core_s, core_r, far_s, far_r, near_s, near_r,
):
    me, across = place()
    tokens, depth = states.shape
    block = depth // 8
    half = block // 2
    count = -(-gate.shape[1] // CUT)
    spare = count * CUT - gate.shape[1]
    outs = (mine_g, mine_u)
    chunks = tokens // SHORT

    def columns(j):
        return pl.ds(pl.multiple_of(j * CUT - j // (count - 1) * spare, 128), CUT)

    def down_load(j):
        slot = lax.rem(j, 2)
        return pltpu.make_async_copy(down.at[columns(j)], downs.at[slot], local.at[3 + slot])

    def inner_load(c, which):
        slot = lax.rem(c, 2)
        part = pl.ds(pl.multiple_of(lax.rem(c, chunks) * SHORT, SHORT), SHORT)
        return pltpu.make_async_copy((gate, up)[which].at[part, columns(c // chunks)], inner.at[slot, which], local.at[5 + 2 * slot + which])

    def inner_back(j):
        down_load(j).wait()

        @pl.when(j + 1 < count)
        def _():
            down_load(j + 1).start()

        @pl.loop(0, chunks)
        def _(r):
            c = chunks * j + r
            slot = lax.rem(c, 2)
            for which in (0, 1):
                inner_load(c, which).wait()

            @pl.when(c + 1 < chunks * count)
            def _():
                for which in (0, 1):
                    inner_load(c + 1, which).start()

            part = pl.ds(pl.multiple_of(r * SHORT, SHORT), SHORT)
            by = dot(outer[part, :], downs[lax.rem(j, 2)], ((1,), (1,))).astype(BF16)
            tiles[0, part, :], tiles[1, part, :] = gates_back(by, inner[slot, 0], inner[slot, 1])

    def rows(number, start=0, size=block):
        return pl.ds(pl.multiple_of(number * block + start, 16), size)

    def core_copy(slot):
        return pltpu.make_async_remote_copy(
            src_ref=core_out.at[slot], dst_ref=core_in.at[slot], send_sem=core_s.at[slot], recv_sem=core_r.at[slot],
            device_id={"dp": across(me, CORE)}, device_id_type=MESH,
        )

    def side_copy(source, target, sent, come, slot, side):
        return pltpu.make_async_remote_copy(
            src_ref=source.at[slot, side], dst_ref=target.at[slot, side], send_sem=sent.at[slot, side], recv_sem=come.at[slot, side],
            device_id={"dp": across(me, (SIDE_X, SIDE_Y)[side])}, device_id_type=MESH,
        )

    def far_copy(slot, side):
        return side_copy(far_out, far_in, far_s, far_r, slot, side)

    def near_copy(slot, side):
        return side_copy(near_out, near_in, near_s, near_r, slot, side)

    blocks = (0, SIDE_X, SIDE_Y, SIDE_X | SIDE_Y)

    def multiply(t, p):
        held = lax.rem(t, HELD)

        @pl.loop(0, depth // TILE)
        def _(i):
            part = pl.ds(pl.multiple_of(i * TILE, TILE), TILE)
            terms[held, part, :] = lax.dot_general(
                states[:, part], tiles[p], (((0,), (0,)), ((), ())), preferred_element_type=F32
            )

    def to_core(t):
        slot, held = lax.rem(t, SLOTS), lax.rem(t, HELD)

        @pl.when(t >= SLOTS)
        def _():
            core_copy(slot).wait_send()

        for i, axes in enumerate(blocks):
            core_out[slot, i] = terms[held, rows(across(me, axes | CORE)), :].astype(BF16)
        core_copy(slot).start()

    def to_far(t):
        slot, held = lax.rem(t, SLOTS), lax.rem(t, HELD)
        core_copy(slot).wait_recv()

        @pl.when(t >= SLOTS)
        def _():
            far_copy(slot, 0).wait_send()
            far_copy(slot, 1).wait_send()

        last = terms[held, rows(across(me, blocks[3])), :] + core_in[slot, 3].astype(F32)
        for side in (0, 1):
            far_out[slot, side] = last[side * half : (side + 1) * half].astype(BF16)
            far_copy(slot, side).start()
        for i, axes in enumerate(blocks[:3]):
            terms[held, rows(across(me, axes)), :] += core_in[slot, i].astype(F32)

    def to_near(t):
        slot, held = lax.rem(t, SLOTS), lax.rem(t, HELD)
        far_copy(slot, 0).wait_recv()
        far_copy(slot, 1).wait_recv()

        @pl.when(t >= SLOTS)
        def _():
            near_copy(slot, 0).wait_send()
            near_copy(slot, 1).wait_send()

        for side in (0, 1):
            number = across(me, (SIDE_X, SIDE_Y)[side])
            extra, plain = (half, 0) if side == 0 else (0, half)
            near_out[slot, side, pl.ds(plain, half)] = terms[held, rows(number, plain, half), :].astype(BF16)
            near_out[slot, side, pl.ds(extra, half)] = (
                terms[held, rows(number, extra, half), :] + far_in[slot, 1 - side].astype(F32)
            ).astype(BF16)
        near_copy(slot, 0).start()
        near_copy(slot, 1).start()

    def to_out(t, p, j):
        slot, held = lax.rem(t, SLOTS), lax.rem(t, HELD)
        near_copy(slot, 0).wait_recv()
        near_copy(slot, 1).wait_recv()
        total = terms[held, rows(me), :] + near_in[slot, 0].astype(F32) + near_in[slot, 1].astype(F32)
        out[p, :, columns(j)] = total.astype(BF16)

    meet(me, across)
    down_load(0).start()
    for which in (0, 1):
        inner_load(0, which).start()
    bring(by_out, outer, local.at[1])
    bring(a, states, local.at[2])

    @pl.loop(0, count + 3)
    def _(j):
        for p in (0, 1):
            t = 2 * j + p

            @pl.when(j < count)
            def _():
                if p == 0:
                    inner_back(j)
                multiply(t, p)

            def stage(lag, run):
                q = (p - lag) % 2
                behind = (lag - p + q) // 2

                @pl.when((j >= behind) & (j - behind < count))
                def _():
                    run(t - lag, q, j - behind)

            stage(5, to_out)
            stage(3, lambda t, q, j: to_near(t))
            stage(1, lambda t, q, j: to_far(t))

            @pl.when(j < count)
            def _():
                to_core(t)

    for slot in range(SLOTS):
        core_copy(slot).wait_send()
        for side in (0, 1):
            far_copy(slot, side).wait_send()
            near_copy(slot, side).wait_send()
    for p in (0, 1):
        bring(out.at[p], outs[p], local.at[2])


def sums(a, by_out, down, gate, up):
    tokens, depth = a.shape
    wide = gate.shape[1]
    block = depth // 8
    anywhere = pl.BlockSpec(memory_space=pl.ANY)
    return pl.pallas_call(
        sums_kernel,
        name="sums",
        out_shape=[jax.ShapeDtypeStruct((block, wide), BF16)] * 2,
        in_specs=[anywhere] * 5,
        out_specs=[anywhere] * 2,
        scratch_shapes=[
            pltpu.VMEM((tokens, depth), BF16), pltpu.VMEM((tokens, depth), BF16), pltpu.VMEM((2, CUT, depth), BF16),
            pltpu.VMEM((2, 2, SHORT, CUT), F32), pltpu.VMEM((2, tokens, CUT), BF16), pltpu.VMEM((HELD, depth, CUT), F32),
            pltpu.VMEM((2, block, wide), BF16),
            pltpu.VMEM((SLOTS, 4, block, CUT), BF16), pltpu.VMEM((SLOTS, 4, block, CUT), BF16),
            pltpu.VMEM((SLOTS, 2, block // 2, CUT), BF16), pltpu.VMEM((SLOTS, 2, block // 2, CUT), BF16),
            pltpu.VMEM((SLOTS, 2, block, CUT), BF16), pltpu.VMEM((SLOTS, 2, block, CUT), BF16),
            pltpu.SemaphoreType.DMA((9,)),
            pltpu.SemaphoreType.DMA((SLOTS,)), pltpu.SemaphoreType.DMA((SLOTS,)),
            pltpu.SemaphoreType.DMA((SLOTS, 2)), pltpu.SemaphoreType.DMA((SLOTS, 2)),
            pltpu.SemaphoreType.DMA((SLOTS, 2)), pltpu.SemaphoreType.DMA((SLOTS, 2)),
        ],
        compiler_params=pltpu.CompilerParams(collective_id=1, has_side_effects=True, vmem_limit_bytes=67_000_000),
        cost_estimate=pl.CostEstimate(flops=6 * tokens * depth * wide, bytes_accessed=100_000_000, transcendentals=0),
    )(a, by_out, down, gate, up)


def solution(mesh):
    def scatter(g):
        return lax.psum_scatter(g, "dp", scatter_dimension=0, tiled=True)

    def step(x, dy, *arrays):
        weights, m, v = (arrays[i : i + 3] for i in (0, 3, 6))
        x, dy = x[0], dy[0]
        _, _, d0, g1, u1, d1, a0, gate0, up0, hidden0, h1, a1, gate1, up1, hidden1 = forward(x, *weights)
        s1 = scale_of(h1)

        rows = ((0,), (0,))
        by_d1 = dot(hidden1, dy, rows).astype(BF16)
        by_d1, dy_, gate1, up1 = after(by_d1, dy, gate1, up1)
        mine_d1 = scatter(by_d1)
        by_hidden1 = dot(dy_, d1, ((1,), (1,))).astype(BF16)
        by_gate1, by_up1 = after(*gates_back(by_hidden1, gate1, up1))
        by_g1 = dot(a1, by_gate1, rows).astype(BF16)
        by_g1, by_gate1, by_up1 = after(by_g1, by_gate1, by_up1)
        mine_g1 = scatter(by_g1)
        by_u1 = dot(a1, by_up1, rows).astype(BF16)
        by_u1, by_gate1, by_up1 = after(by_u1, by_gate1, by_up1)
        mine_u1 = scatter(by_u1)
        by_a1 = dot(by_gate1, g1, ((1,), (1,))).astype(BF16) + dot(by_up1, u1, ((1,), (1,))).astype(BF16)
        by_h1 = norm_back(by_a1, h1, s1).astype(BF16) + dy
        (by_h1,) = after(by_h1)
        by_d0 = dot(hidden0, by_h1, rows).astype(BF16)
        by_d0, by_h1, gate0, up0 = after(by_d0, by_h1, gate0, up0)
        mine_d0 = scatter(by_d0)
        mine_g0, mine_u0 = sums(a0, by_h1, d0, gate0, up0)

        gradients = [jnp.stack(pair).astype(F32) for pair in ((mine_g0, mine_g1), (mine_u0, mine_u1), (mine_d0, mine_d1))]
        new = [adamw(w.astype(F32), m, v, g) for w, m, v, g in zip(weights, m, v, gradients, strict=True)]
        return tuple(one[which] for which in range(3) for one in new)

    states, cut = P(("rep", "dp"), None, None), P(None, "dp", None)
    return jax.shard_map(
        step,
        mesh=mesh,
        in_specs=(states, states) + (cut,) * 9,
        out_specs=(P("rep", "dp", None),) * 9,
        check_vma=False,
    )
```
